32 devices in a mesh: gx: 4 (over y, core), gy: 4 (over z), gz: 2 (over x).
Axes of the slice: x: 2, y: 2, z: 4, core: 2. Of those that a mesh axis runs over, the one named last changes fastest.
Arguments:
- moments: float32 [8, 16, 64, 1024], P(None, 'gx', 'gy', 'gz'), may hold values from 0.001 to 60, as said below
- velocity: float32 [3, 16, 64, 1024], P(None, 'gx', 'gy', 'gz'), may hold values from -4 to 4
- drift: float32 [3, 16, 64, 1024], P(None, 'gx', 'gy', 'gz'), may hold values from -8 to 8
Outputs:
- updated: float32 [8, 16, 64, 1024], P(None, 'gx', 'gy', 'gz')
- totals: float32 [8], replicated
The draws below stay inside these ranges and needn't reach their ends.
Inputs may be any that keep to these rules, and one draw needn't show every extreme that they name: In every cell the 8 entries are the moments of order 0 to 7 of a log-normal distribution of particle size.
All inputs are finite; a program needn't handle non-finite values. Where the reference program divides by a largest or mean magnitude, that divisor is 1e-20 or more.
Results may differ from the reference program's by a relative error of at most 0.0003.
Values sent between devices are 32-bit elements; how exact they have to be, the bound alone decides.
A program may use at most 64 MiB of HBM per device.

```python
import jax
import jax.numpy as jnp
from jax import lax

SWEEPS = 6
NX = 16
NY = 64
NZ = 1024


def draw_moments(key, part):
    keys = jax.random.split(key, 3)
    shape = (NX, NY, NZ)
    place_x = lax.broadcasted_iota(jnp.float32, shape, 0) / NX
    place_y = lax.broadcasted_iota(jnp.float32, shape, 1) / NY
    place_z = lax.broadcasted_iota(jnp.float32, shape, 2) / NZ
    ramp = 1.0 + 2.0 * (place_x + place_y + place_z) / 3.0
    rough = jnp.exp(jax.random.uniform(keys[0], shape, jnp.float32, -0.35, 0.35))
    width = jax.random.uniform(keys[1], shape, jnp.float32, 0.3, 0.8)
    offset = jax.random.uniform(keys[2], shape, jnp.float32, -0.2, 0.2)
    number = ramp * rough
    variance = width * width
    center = -3.5 * variance + offset
    orders = jnp.arange(8, dtype=jnp.float32)[:, None, None, None]
    return number[None] * jnp.exp(orders * center[None] + 0.5 * orders * orders * variance[None])


def shard_levels(own_key, shape, pieces, smallest, top_value):
    level, own = 1.0, jax.random.fold_in(own_key, 6)
    for position, shards_of in pieces:
        heights = jnp.exp(jax.random.uniform(jax.random.fold_in(own, position), (shards_of,), jnp.float32, smallest / len(pieces), top_value / len(pieces)))
        level = level * jnp.repeat(heights, shape[position] // shards_of).reshape([-1 if axis == position else 1 for axis in range(len(shape))])
    return level


def scatter_about(own_key, dims, scale, reach, cuts=(), kind=jnp.bfloat16):
    array = scale * jax.random.normal(own_key, dims, jnp.float32)
    if cuts:
        array = array * shard_levels(own_key, dims, cuts, -0.22, 0.18)
    return jnp.clip(array, -reach, reach).astype(kind)


def setup_inputs(seed: int = 0) -> dict:
    splits = jax.random.split(jax.random.key(seed), 4)
    return {
        "moments": draw_moments(jax.random.fold_in(splits[3], 71), 0),
        "velocity": scatter_about(splits[1], (3, NX, NY, NZ), 1.0, 4.0, ((1, 4), (2, 4), (3, 2)), jnp.float32),
        "drift": scatter_about(splits[2], (3, NX, NY, NZ), 2.0, 8.0, ((1, 4), (2, 4), (3, 2)), jnp.float32),
    }


cfl_number = 0.4
speed_eps = 1e-06
pair_list = ((0, 1), (0, 2), (0, 3), (1, 2), (1, 3), (2, 3))

def entry_key(first_index, second_index):
    return (min(first_index, second_index), max(first_index, second_index))

def invert(moment):
    levels = [moment[order] for order in range(8)]
    zeros = jnp.zeros_like(levels[0])
    before = [zeros] * 8
    alphas = [levels[1] / levels[0]]
    betas = [levels[0]]
    for level in range(1, 4):
        fresh = [zeros] * 8
        for column in range(level, 8 - level):
            fresh[column] = levels[column + 1] - alphas[level - 1] * levels[column] - betas[level - 1] * before[column]
        alphas.append(fresh[level + 1] / fresh[level] - levels[level] / levels[level - 1])
        betas.append(fresh[level] / levels[level - 1])
        before, levels = (levels, fresh)
    table = {}
    for row_index in range(4):
        for col_index in range(row_index, 4):
            table[row_index, col_index] = zeros
    for row_index in range(4):
        table[row_index, row_index] = alphas[row_index]
    for row_index in range(3):
        table[row_index, row_index + 1] = jnp.sqrt(betas[row_index + 1])
    first = [jnp.ones_like(zeros), zeros, zeros, zeros]
    for _ in range(SWEEPS):
        for pivot, other in pair_list:
            coupling = table[pivot, other]
            head = table[pivot, pivot]
            tail = table[other, other]
            spread = tail - head
            orient = jnp.where(spread >= 0, 1.0, -1.0)
            tangent = orient * 2.0 * coupling / (jnp.abs(spread) + jnp.sqrt(spread * spread + 4.0 * coupling * coupling))
            cosine = 1.0 / jnp.sqrt(1.0 + tangent * tangent)
            sine = tangent * cosine
            for rest in range(4):
                if rest != pivot and rest != other:
                    near = table[entry_key(rest, pivot)]
                    far = table[entry_key(rest, other)]
                    table[entry_key(rest, pivot)] = cosine * near - sine * far
                    table[entry_key(rest, other)] = sine * near + cosine * far
            table[pivot, pivot] = head - tangent * coupling
            table[other, other] = tail + tangent * coupling
            table[pivot, other] = jnp.zeros_like(coupling)
            first_p = first[pivot]
            first_q = first[other]
            first[pivot] = cosine * first_p - sine * first_q
            first[other] = sine * first_p + cosine * first_q
    weights = [moment[0] * first[node] * first[node] for node in range(4)]
    places = [table[node, node] for node in range(4)]
    return jnp.stack(weights + places)

def face_flux(extended, axis, count):

    def part(channel, start):
        return lax.slice_in_dim(extended[channel], start, start + count + 1, axis=axis - 1)
    mean_speed = 0.5 * (part(8, 0) + part(8, 1))
    mean_drift = 0.5 * (part(9, 0) + part(9, 1))
    zeros = jnp.zeros_like(mean_speed)
    accum = [zeros] * 8
    for node in range(4):
        for start, upwind in ((0, jnp.maximum), (1, jnp.minimum)):
            size = part(4 + node, start)
            carried = part(node, start) * upwind(mean_speed + mean_drift * size, 0.0)
            for order in range(8):
                accum[order] = accum[order] + carried
                carried = carried * size
    return jnp.stack(accum)

def reference(moments, velocity, drift):
    nodes = jnp.moveaxis(lax.map(invert, jnp.moveaxis(moments, 1, 0)), 0, 1)
    change = jnp.zeros_like(moments)
    for direction in range(3):
        axis = direction + 1
        count = moments.shape[axis]
        pack = jnp.concatenate([nodes, velocity[direction:direction + 1], drift[direction:direction + 1]], 0)
        widths = [(0, 0), (0, 0), (0, 0), (0, 0)]
        widths[axis] = (1, 1)
        if direction < 2:
            extended = jnp.pad(pack, widths, mode='wrap')
        else:
            extended = jnp.pad(pack, widths)
        flux = face_flux(extended, axis, count)
        if direction == 2:
            face = lax.broadcasted_iota(jnp.int32, flux.shape, 3)
            flux = jnp.where((face == 0) | (face == count), 0.0, flux)
        change = change + lax.slice_in_dim(flux, 1, count + 1, axis=axis) - lax.slice_in_dim(flux, 0, count, axis=axis)
    speed = jnp.zeros_like(moments[0])
    for direction in range(3):
        speed = speed + lax.optimization_barrier(jnp.max(jnp.abs(velocity[direction][None] + drift[direction][None] * nodes[4:8]), axis=0))
    step_size = cfl_number / (jnp.max(speed) + speed_eps)
    updated = moments - step_size * change
    totals = lax.optimization_barrier(jnp.sum(updated, axis=(1, 2, 3))) / (NX * NY * NZ)
    return (updated, totals)
```

```python
import functools

import jax
import jax.numpy as jnp
from jax import lax
from jax.experimental import pallas as pl
from jax.experimental.pallas import tpu as pltpu
from jax.sharding import PartitionSpec as P

SWEEPS = 6
AXES = ("gx", "gy", "gz")
JACOBI_LANES = 256
LANES = 128

cfl_number = 0.4
speed_eps = 1e-06
pair_list = ((0, 1), (0, 2), (0, 3), (1, 2), (1, 3), (2, 3))


def entry_key(i, j):
    return (min(i, j), max(i, j))


def rotated(cosine, sine, near, far):
    if near is None and far is None:
        return None, None
    if near is None:
        return -(sine * far), cosine * far
    if far is None:
        return cosine * near, sine * near
    return cosine * near - sine * far, sine * near + cosine * far


def invert(moment):
    levels = list(moment)
    before = None
    inverse = 1.0 / levels[0]
    ratios = [levels[1] * inverse]
    alphas = [ratios[0]]
    betas = [levels[0]]
    for level in range(1, 4):
        fresh = [None] * 8
        for column in range(level, 8 - level):
            value = levels[column + 1] - alphas[level - 1] * levels[column]
            if level > 1:
                value = value - betas[level - 1] * before[column]
            fresh[column] = value
        betas.append(fresh[level] * inverse)
        inverse = 1.0 / fresh[level]
        ratios.append(fresh[level + 1] * inverse)
        alphas.append(ratios[level] - ratios[level - 1])
        before, levels = levels, fresh
    table = {(i, j): None for i in range(4) for j in range(i, 4)}
    for i in range(4):
        table[i, i] = alphas[i]
    for i in range(3):
        table[i, i + 1] = jnp.sqrt(betas[i + 1])
    first = [1.0, None, None, None]
    for _ in range(SWEEPS):
        for p, q in pair_list:
            coupling = table[p, q]
            if coupling is None:
                continue
            spread = table[q, q] - table[p, p]
            double = coupling + coupling
            r = lax.rsqrt(spread * spread + double * double)
            c2 = 0.5 + 0.5 * (jnp.abs(spread) * r)
            rc = lax.rsqrt(c2)
            cosine = c2 * rc
            signed = jnp.where(spread >= 0, coupling, -coupling)
            sine = signed * (r * rc)
            shift = sine * rc * coupling
            for rest in range(4):
                if rest not in (p, q):
                    a, b = entry_key(rest, p), entry_key(rest, q)
                    table[a], table[b] = rotated(cosine, sine, table[a], table[b])
            table[p, p] = table[p, p] - shift
            table[q, q] = table[q, q] + shift
            table[p, q] = None
            first[p], first[q] = rotated(cosine, sine, first[p], first[q])
    weights = [moment[0] * first[i] * first[i] for i in range(4)]
    return weights, [table[i, i] for i in range(4)]


def outflow(weights, sizes, mean_speed, mean_drift, upwind):
    sums = None
    for w, s in zip(weights, sizes):
        term = w * upwind(mean_speed + mean_drift * s, 0.0)
        terms = [term]
        for _ in range(7):
            term = term * s
            terms.append(term)
        sums = terms if sums is None else [a + b for a, b in zip(sums, terms)]
    return sums


def kernel(
    sizes, m_hbm, v_hbm, g_hbm, out_hbm, tot_ref,
    m, v, g, nodes, acc, out, xp, xm, zp, zm,
    hvx, vy_s, vy_r, vz_s, vz_r, y_s, y_r, z_s, z_r, peak, total,
    in_sem, out_sem, nb_send, nb_recv, all_send, all_recv,
):
    X, Y, Z = m.shape[1:]
    count = sizes[0] * sizes[1] * sizes[2]
    at = [lax.axis_index(a) for a in AXES]
    me = (at[0] * sizes[1] + at[1]) * sizes[2] + at[2]
    row = lax.broadcasted_iota(jnp.int32, (Y, LANES), 0)
    lane = lax.broadcasted_iota(jnp.int32, (Y, LANES), 1)
    bottom = at[2] == 0
    top = at[2] == sizes[2] - 1

    def peer(offset):
        where = lax.rem(me + offset, count)
        return (
            where // (sizes[1] * sizes[2]),
            lax.rem(where // sizes[2], sizes[1]),
            lax.rem(where, sizes[2]),
        )

    def beside(axis, step):
        place = list(at)
        place[axis] = lax.rem(at[axis] + step + sizes[axis], sizes[axis])
        return tuple(place)

    loads = [pltpu.make_async_copy(m_hbm.at[:, x], m.at[:, x], in_sem.at[x]) for x in range(X)]
    loads_v = pltpu.make_async_copy(v_hbm, v, in_sem.at[X])
    loads_g = pltpu.make_async_copy(g_hbm, g, in_sem.at[X + 1])
    loads_v.start()
    loads_g.start()
    edge = [0] if X == 1 else [0, X - 1]
    inner = list(range(1, X - 1))
    for x in edge + inner:
        loads[x].start()

    barrier = pltpu.get_barrier_semaphore()

    def greet(offset, carry):
        pl.semaphore_signal(
            barrier, inc=1, device_id=peer(offset), device_id_type=pl.DeviceIdType.MESH
        )
        return carry

    lax.fori_loop(1, count, greet, 0)

    sent = []

    def send(src, dst, axis, step):
        index = len(sent)
        copy = pltpu.make_async_remote_copy(
            src_ref=src, dst_ref=dst, send_sem=nb_send.at[index], recv_sem=nb_recv.at[index],
            device_id=beside(axis, step), device_id_type=pl.DeviceIdType.MESH,
        )
        copy.start()
        sent.append(copy)
        return copy

    loads_v.wait()
    loads_g.wait()
    for x in range(X):
        for part, ref in ((0, v), (1, g)):
            vy_s[0, x, part : part + 1, :] = ref[1, x, Y - 1 : Y, :]
            vy_s[1, x, part : part + 1, :] = ref[1, x, 0:1, :]
        high = [ref[2, x, :, Z - LANES : Z] for ref in (v, g)]
        low = [ref[2, x, :, 0:LANES] for ref in (v, g)]
        vz_s[0, x] = jnp.where(lane == 0, pltpu.roll(high[0], 1, 1), pltpu.roll(high[1], 2, 1))
        vz_s[1, x] = jnp.where(lane == 0, low[0], pltpu.roll(low[1], 1, 1))

    pl.semaphore_wait(barrier, count - 1)
    velocity_copies = [
        send(v.at[0, X - 1], hvx.at[0, 0], 0, 1),
        send(g.at[0, X - 1], hvx.at[0, 1], 0, 1),
        send(v.at[0, 0], hvx.at[1, 0], 0, -1),
        send(g.at[0, 0], hvx.at[1, 1], 0, -1),
        send(vy_s.at[0], vy_r.at[0], 1, 1),
        send(vy_s.at[1], vy_r.at[1], 1, -1),
        send(vz_s.at[0], vz_r.at[0], 2, 1),
        send(vz_s.at[1], vz_r.at[1], 2, -1),
    ]

    chunks = Z // JACOBI_LANES

    def solve(x, chunk, best):
        zs = pl.ds(pl.multiple_of(chunk * JACOBI_LANES, JACOBI_LANES), JACOBI_LANES)
        weights, places = invert([m[k, x, :, zs] for k in range(8)])
        for i in range(4):
            nodes[i, x, :, zs] = weights[i]
            nodes[4 + i, x, :, zs] = places[i]
        speed = None
        for d in range(3):
            vd, gd = v[d, x, :, zs], g[d, x, :, zs]
            parts = [jnp.abs(vd + gd * s) for s in places]
            largest = jnp.maximum(
                jnp.maximum(parts[0], parts[1]), jnp.maximum(parts[2], parts[3])
            )
            speed = largest if speed is None else speed + largest
        return jnp.maximum(best, speed)

    best = jnp.zeros((Y, JACOBI_LANES), jnp.float32)
    for x in edge:
        loads[x].wait()
    best = lax.fori_loop(
        0, len(edge) * chunks,
        lambda i, b: solve(lax.div(i, chunks) * (X - 1), lax.rem(i, chunks), b), best,
    )

    for copy in velocity_copies[:4]:
        copy.wait_recv()

    def lanes_of(chunk):
        return pl.ds(pl.multiple_of(chunk * LANES, LANES), LANES)

    def nodes_of(x, zs):
        return (
            [nodes[i, x, :, zs] for i in range(4)], [nodes[4 + i, x, :, zs] for i in range(4)]
        )

    def edge_x(chunk, carry):
        zs = lanes_of(chunk)
        w, s = nodes_of(X - 1, zs)
        speed = 0.5 * (v[0, X - 1, :, zs] + hvx[1, 0, :, zs])
        slope = 0.5 * (g[0, X - 1, :, zs] + hvx[1, 1, :, zs])
        for k, value in enumerate(outflow(w, s, speed, slope, jnp.maximum)):
            xp[X, k, :, zs] = value
        w, s = nodes_of(0, zs)
        speed = 0.5 * (v[0, 0, :, zs] + hvx[0, 0, :, zs])
        slope = 0.5 * (g[0, 0, :, zs] + hvx[0, 1, :, zs])
        for k, value in enumerate(outflow(w, s, speed, slope, jnp.minimum)):
            xm[0, k, :, zs] = value
        return carry

    lax.fori_loop(0, Z // LANES, edge_x, 0)
    x_copies = [
        send(xp.at[X], xp.at[0], 0, 1),
        send(xm.at[0], xm.at[X], 0, -1),
    ]

    for x in inner:
        loads[x].wait()
    if inner:
        best = lax.fori_loop(
            0, len(inner) * chunks,
            lambda i, b: solve(lax.div(i, chunks) + 1, lax.rem(i, chunks), b), best,
        )

    best = jnp.max(best, axis=0, keepdims=True)
    best = functools.reduce(
        jnp.maximum, [best[:, i : i + LANES] for i in range(0, JACOBI_LANES, LANES)]
    )
    peak[0] = best

    def spread_copy(buffer, which, offset):
        return pltpu.make_async_remote_copy(
            src_ref=buffer.at[0], dst_ref=buffer.at[offset],
            send_sem=all_send.at[which, offset], recv_sem=all_recv.at[which, offset],
            device_id=peer(offset), device_id_type=pl.DeviceIdType.MESH,
        )

    def spread(buffer, which):
        def one(offset, carry):
            spread_copy(buffer, which, offset).start()
            return carry

        lax.fori_loop(1, count, one, 0)

    def gathered(buffer, which):
        def one(offset, carry):
            spread_copy(buffer, which, offset).wait_recv()
            return carry

        lax.fori_loop(1, count, one, 0)

    for copy in velocity_copies[4:]:
        copy.wait_recv()

    zc = Z // LANES

    def side_faces(i, carry):
        x, chunk = lax.div(i, zc), lax.rem(i, zc)
        zs = lanes_of(chunk)
        w, s = nodes_of(x, zs)
        vy, gy = v[1, x, :, zs], g[1, x, :, zs]
        up = [
            jnp.where(row == Y - 1, vy_r[1, x, part : part + 1, zs], pltpu.roll(a, Y - 1, 0))
            for part, a in ((0, vy), (1, gy))
        ]
        down = [
            jnp.where(row == 0, vy_r[0, x, part : part + 1, zs], pltpu.roll(a, 1, 0))
            for part, a in ((0, vy), (1, gy))
        ]
        high = outflow(w, s, 0.5 * (vy + up[0]), 0.5 * (gy + up[1]), jnp.maximum)
        for k in range(8):
            y_s[0, x, k : k + 1, zs] = high[k][Y - 1 : Y, :]
            acc[x, k, :, zs] = high[k] - jnp.where(row == 0, 0.0, pltpu.roll(high[k], 1, 0))
        low = outflow(w, s, 0.5 * (vy + down[0]), 0.5 * (gy + down[1]), jnp.minimum)
        for k in range(8):
            y_s[1, x, k : k + 1, zs] = low[k][0:1, :]
            acc[x, k, :, zs] += (
                jnp.where(row == Y - 1, 0.0, pltpu.roll(low[k], Y - 1, 0)) - low[k]
            )
        return carry

    lax.fori_loop(0, X * zc, side_faces, 0)
    spread(peak, 0)
    y_copies = [send(y_s.at[0], y_r.at[0], 1, 1), send(y_s.at[1], y_r.at[1], 1, -1)]

    def wall_faces(i, carry):
        x, chunk = lax.div(i, zc), lax.rem(i, zc)
        zs = lanes_of(chunk)
        nxt = lanes_of(lax.rem(chunk + 1, zc))
        prv = lanes_of(lax.rem(chunk + zc - 1, zc))
        w, s = nodes_of(x, zs)
        final = chunk == zc - 1
        start = chunk == 0

        def means(ref, part):
            here = ref[2, x, :, zs]
            after = jnp.where(final, pltpu.roll(vz_r[1, x], LANES - part, 1), ref[2, x, :, nxt])
            ahead = jnp.where(
                start, pltpu.roll(vz_r[0, x], LANES - 1 - part, 1), ref[2, x, :, prv]
            )
            up = jnp.where(
                lane == LANES - 1, pltpu.roll(after, LANES - 1, 1), pltpu.roll(here, LANES - 1, 1)
            )
            down = jnp.where(lane == 0, pltpu.roll(ahead, 1, 1), pltpu.roll(here, 1, 1))
            return 0.5 * (here + up), 0.5 * (here + down)

        speeds, slopes = means(v, 0), means(g, 1)
        shut_high = (lane == LANES - 1) & (final & top)
        shut_low = (lane == 0) & (start & bottom)
        high = outflow(w, s, speeds[0], slopes[0], jnp.maximum)
        for k in range(8):
            zp[x, k, :, zs] = jnp.where(shut_high, 0.0, high[k])
        low = outflow(w, s, speeds[1], slopes[1], jnp.minimum)
        for k in range(8):
            zm[x, k, :, zs] = jnp.where(shut_low, 0.0, low[k])
        return carry

    lax.fori_loop(0, X * zc, wall_faces, 0)

    def pack_z(x, carry):
        high = jnp.zeros((Y, LANES), jnp.float32)
        low = jnp.zeros((Y, LANES), jnp.float32)
        for k in range(8):
            high = jnp.where(
                lane == k, pltpu.roll(zp[x, k, :, Z - LANES : Z], k + 1, 1), high
            )
            column = zm[x, k, :, 0:LANES]
            low = jnp.where(lane == k, pltpu.roll(column, k, 1) if k else column, low)
        z_s[0, x] = high
        z_s[1, x] = low
        return carry

    lax.fori_loop(0, X, pack_z, 0)

    def inner_x(i, carry):
        x, chunk = lax.div(i, zc), lax.rem(i, zc)
        zs = lanes_of(chunk)
        speed = 0.5 * (v[0, x, :, zs] + v[0, x + 1, :, zs])
        slope = 0.5 * (g[0, x, :, zs] + g[0, x + 1, :, zs])
        w, s = nodes_of(x, zs)
        left = outflow(w, s, speed, slope, jnp.maximum)
        for k in range(8):
            xp[x + 1, k, :, zs] = left[k]
        w, s = nodes_of(x + 1, zs)
        right = outflow(w, s, speed, slope, jnp.minimum)
        for k in range(8):
            xm[x + 1, k, :, zs] = right[k]
        return carry

    z_copies = [send(z_s.at[0], z_r.at[0], 2, 1), send(z_s.at[1], z_r.at[1], 2, -1)]
    if X > 1:
        lax.fori_loop(0, (X - 1) * zc, inner_x, 0)

    gathered(peak, 0)
    largest = jnp.max(jnp.max(peak[...], axis=0), axis=1, keepdims=True)
    step = cfl_number / (largest + speed_eps)

    for copy in x_copies + y_copies + z_copies:
        copy.wait_recv()

    wide_row = lax.broadcasted_iota(jnp.int32, (Y, Z), 0)
    wide_lane = lax.broadcasted_iota(jnp.int32, (Y, Z), 1)

    def combine(x, sums):
        fresh = []
        low_all, high_all = z_r[0, x], z_r[1, x]
        for k in range(8):
            fp, fm = zp[x, k], zm[x, k]
            before = jnp.where(wide_lane == 0, 0.0, pltpu.roll(fp, 1, 1))
            after = jnp.where(wide_lane == Z - 1, 0.0, pltpu.roll(fm, Z - 1, 1))
            change = acc[x, k] + ((fp + after) - (fm + before))
            change = change + ((xp[x + 1, k] + xm[x + 1, k]) - (xp[x, k] + xm[x, k]))
            change = change + jnp.where(
                wide_row == Y - 1, y_r[1, x, k : k + 1, :],
                jnp.where(wide_row == 0, -y_r[0, x, k : k + 1, :], 0.0),
            )
            out[k, x] = m[k, x] - step * change
            first = jnp.where(lane == 0, pltpu.roll(low_all, LANES - k, 1) if k else low_all, 0.0)
            last = jnp.where(lane == LANES - 1, pltpu.roll(high_all, LANES - 1 - k, 1), 0.0)
            out[k, x, :, 0:LANES] += step * first
            out[k, x, :, Z - LANES : Z] -= step * last
            value = out[k, x]
            fold = functools.reduce(
                jnp.add, [value[i : i + 8, :] for i in range(0, Y, 8)]
            )
            fold = functools.reduce(
                jnp.add, [fold[:, i : i + LANES] for i in range(0, Z, LANES)]
            )
            fresh.append(sums[k] + fold)
        pltpu.make_async_copy(out.at[:, x], out_hbm.at[:, x], out_sem.at[x]).start()
        return tuple(fresh)

    zero = jnp.zeros((8, LANES), jnp.float32)
    sums = lax.fori_loop(0, X, combine, (zero,) * 8)

    one_lane = lax.broadcasted_iota(jnp.int32, (1, LANES), 1)
    packed = jnp.zeros((1, LANES), jnp.float32)
    for k in range(8):
        value = jnp.sum(jnp.sum(sums[k], axis=0, keepdims=True), axis=1, keepdims=True)
        packed = jnp.where(one_lane == k, value, packed)
    total[0] = packed
    spread(total, 1)
    gathered(total, 1)
    tot_ref[...] = jnp.sum(total[...], axis=0) / float(count * X * Y * Z)

    for x in range(X):
        pltpu.make_async_copy(out.at[:, x], out_hbm.at[:, x], out_sem.at[x]).wait()
    for copy in sent:
        copy.wait_send()

    def drain(offset, carry):
        for which, buffer in ((0, peak), (1, total)):
            spread_copy(buffer, which, offset).wait_send()
        return carry

    lax.fori_loop(1, count, drain, 0)


def shards(sizes, moments, velocity, drift):
    _, X, Y, Z = moments.shape
    count = sizes[0] * sizes[1] * sizes[2]
    f32 = jnp.float32
    vm = lambda *shape: pltpu.VMEM(shape, f32)
    updated, totals = pl.pallas_call(
        functools.partial(kernel, sizes),
        name="transport",
        out_shape=(
            jax.ShapeDtypeStruct(moments.shape, f32), jax.ShapeDtypeStruct((1, LANES), f32)
        ),
        in_specs=[pl.BlockSpec(memory_space=pl.ANY)] * 3,
        out_specs=(
            pl.BlockSpec(memory_space=pl.ANY), pl.BlockSpec(memory_space=pltpu.VMEM)
        ),
        scratch_shapes=[
            vm(8, X, Y, Z), vm(3, X, Y, Z), vm(3, X, Y, Z), vm(8, X, Y, Z), vm(X, 8, Y, Z),
            vm(8, X, Y, Z), vm(X + 1, 8, Y, Z), vm(X + 1, 8, Y, Z), vm(X, 8, Y, Z),
            vm(X, 8, Y, Z),
            vm(2, 2, Y, Z), vm(2, X, 2, Z), vm(2, X, 2, Z), vm(2, X, Y, LANES),
            vm(2, X, Y, LANES), vm(2, X, 8, Z), vm(2, X, 8, Z), vm(2, X, Y, LANES),
            vm(2, X, Y, LANES), vm(count, 1, LANES), vm(count, 1, LANES),
            pltpu.SemaphoreType.DMA((X + 2,)), pltpu.SemaphoreType.DMA((X,)),
            pltpu.SemaphoreType.DMA((14,)), pltpu.SemaphoreType.DMA((14,)),
            pltpu.SemaphoreType.DMA((2, count)), pltpu.SemaphoreType.DMA((2, count)),
        ],
        compiler_params=pltpu.CompilerParams(collective_id=0, has_side_effects=True),
    )(moments, velocity, drift)
    return updated, totals[0, :8]


def solution(mesh):
    spec = P(None, "gx", "gy", "gz")
    sizes = tuple(mesh.shape[a] for a in AXES)
    return jax.shard_map(
        functools.partial(shards, sizes), mesh=mesh, in_specs=(spec,) * 3,
        out_specs=(spec, P()), check_vma=False,
    )
```

```python
import functools

import jax
import jax.numpy as jnp
from jax import lax
from jax.experimental import pallas as pl
from jax.experimental.pallas import tpu as pltpu
from jax.sharding import PartitionSpec as P

SWEEPS = 6
AXES = ("gx", "gy", "gz")
JACOBI_LANES = 256
LANES = 128

cfl_number = 0.4
speed_eps = 1e-06
pair_list = ((0, 1), (0, 2), (0, 3), (1, 2), (1, 3), (2, 3))


def entry_key(i, j):
    return (min(i, j), max(i, j))


def rotated(cosine, sine, near, far):
    if near is None and far is None:
        return None, None
    if near is None:
        return -(sine * far), cosine * far
    if far is None:
        return cosine * near, sine * near
    return cosine * near - sine * far, sine * near + cosine * far


def invert(moment):
    levels = list(moment)
    before = None
    inverse = 1.0 / levels[0]
    ratios = [levels[1] * inverse]
    alphas = [ratios[0]]
    betas = [levels[0]]
    for level in range(1, 4):
        fresh = [None] * 8
        for column in range(level, 8 - level):
            value = levels[column + 1] - alphas[level - 1] * levels[column]
            if level > 1:
                value = value - betas[level - 1] * before[column]
            fresh[column] = value
        betas.append(fresh[level] * inverse)
        inverse = 1.0 / fresh[level]
        ratios.append(fresh[level + 1] * inverse)
        alphas.append(ratios[level] - ratios[level - 1])
        before, levels = levels, fresh
    table = {(i, j): None for i in range(4) for j in range(i, 4)}
    for i in range(4):
        table[i, i] = alphas[i]
    for i in range(3):
        table[i, i + 1] = jnp.sqrt(betas[i + 1])
    first = [1.0, None, None, None]
    for _ in range(SWEEPS):
        for p, q in pair_list:
            coupling = table[p, q]
            if coupling is None:
                continue
            spread = table[q, q] - table[p, p]
            double = coupling + coupling
            r = lax.rsqrt(spread * spread + double * double)
            c2 = 0.5 + 0.5 * (jnp.abs(spread) * r)
            rc = lax.rsqrt(c2)
            cosine = c2 * rc
            signed = jnp.where(spread >= 0, coupling, -coupling)
            sine = signed * (r * rc)
            shift = sine * rc * coupling
            for rest in range(4):
                if rest not in (p, q):
                    a, b = entry_key(rest, p), entry_key(rest, q)
                    table[a], table[b] = rotated(cosine, sine, table[a], table[b])
            table[p, p] = table[p, p] - shift
            table[q, q] = table[q, q] + shift
            table[p, q] = None
            first[p], first[q] = rotated(cosine, sine, first[p], first[q])
    weights = [moment[0] * first[i] * first[i] for i in range(4)]
    return weights, [table[i, i] for i in range(4)]


def outflow(weights, sizes, mean_speed, mean_drift, upwind):
    sums = None
    for w, s in zip(weights, sizes):
        term = w * upwind(mean_speed + mean_drift * s, 0.0)
        terms = [term]
        for _ in range(7):
            term = term * s
            terms.append(term)
        sums = terms if sums is None else [a + b for a, b in zip(sums, terms)]
    return sums


def kernel(
    sizes, m_hbm, v_hbm, g_hbm, out, tot_ref,
    m, v, g, nodes, acc, fx, zp, zm,
    hvx, vy_s, vy_r, vz_s, vz_r, y_s, y_r, z_s, z_r, peak, total,
    in_sem, nb_send, nb_recv, all_send, all_recv,
):
    X, Y, Z = m.shape[1:]
    count = sizes[0] * sizes[1] * sizes[2]
    at = [lax.axis_index(a) for a in AXES]
    me = (at[0] * sizes[1] + at[1]) * sizes[2] + at[2]
    row = lax.broadcasted_iota(jnp.int32, (Y, LANES), 0)
    lane = lax.broadcasted_iota(jnp.int32, (Y, LANES), 1)
    bottom = at[2] == 0
    top = at[2] == sizes[2] - 1

    def peer(offset):
        where = lax.rem(me + offset, count)
        return (
            where // (sizes[1] * sizes[2]),
            lax.rem(where // sizes[2], sizes[1]),
            lax.rem(where, sizes[2]),
        )

    def beside(axis, step):
        place = list(at)
        place[axis] = lax.rem(at[axis] + step + sizes[axis], sizes[axis])
        return tuple(place)

    loads = [pltpu.make_async_copy(m_hbm.at[:, x], m.at[:, x], in_sem.at[x]) for x in range(X)]
    loads_v = pltpu.make_async_copy(v_hbm, v, in_sem.at[X])
    loads_g = pltpu.make_async_copy(g_hbm, g, in_sem.at[X + 1])
    edge = [0] if X == 1 else [0, X - 1]
    inner = list(range(1, X - 1))
    loads[0].start()
    loads_v.start()
    loads_g.start()
    for x in edge[1:] + inner:
        loads[x].start()

    barrier = pltpu.get_barrier_semaphore()

    def greet(offset, carry):
        pl.semaphore_signal(
            barrier, inc=1, device_id=peer(offset), device_id_type=pl.DeviceIdType.MESH
        )
        return carry

    lax.fori_loop(1, count, greet, 0)

    sent = []

    def send(src, dst, axis, step):
        index = len(sent)
        copy = pltpu.make_async_remote_copy(
            src_ref=src, dst_ref=dst, send_sem=nb_send.at[index], recv_sem=nb_recv.at[index],
            device_id=beside(axis, step), device_id_type=pl.DeviceIdType.MESH,
        )
        copy.start()
        sent.append(copy)
        return copy

    loads_v.wait()
    loads_g.wait()
    for x in range(X):
        for part, ref in ((0, v), (1, g)):
            vy_s[0, x, part : part + 1, :] = ref[1, x, Y - 1 : Y, :]
            vy_s[1, x, part : part + 1, :] = ref[1, x, 0:1, :]
        high = [ref[2, x, :, Z - LANES : Z] for ref in (v, g)]
        low = [ref[2, x, :, 0:LANES] for ref in (v, g)]
        vz_s[0, x] = jnp.where(lane == 0, pltpu.roll(high[0], 1, 1), pltpu.roll(high[1], 2, 1))
        vz_s[1, x] = jnp.where(lane == 0, low[0], pltpu.roll(low[1], 1, 1))

    chunks = Z // JACOBI_LANES

    def solve(x, chunk, best):
        zs = pl.ds(pl.multiple_of(chunk * JACOBI_LANES, JACOBI_LANES), JACOBI_LANES)
        weights, places = invert([m[k, x, :, zs] for k in range(8)])
        for i in range(4):
            nodes[x + 1, i, :, zs] = weights[i]
            nodes[x + 1, 4 + i, :, zs] = places[i]
        speed = None
        for d in range(3):
            vd, gd = v[d, x, :, zs], g[d, x, :, zs]
            parts = [jnp.abs(vd + gd * s) for s in places]
            largest = jnp.maximum(
                jnp.maximum(parts[0], parts[1]), jnp.maximum(parts[2], parts[3])
            )
            speed = largest if speed is None else speed + largest
        return jnp.maximum(best, speed)

    best = jnp.zeros((Y, JACOBI_LANES), jnp.float32)
    def solve_layer(x, best):
        return lax.fori_loop(0, chunks, lambda i, b: solve(x, i, b), best)

    loads[0].wait()
    best = solve_layer(0, best)
    pl.semaphore_wait(barrier, count - 1)
    velocity_copies = [
        send(v.at[0, X - 1], hvx.at[0, 0], 0, 1),
        send(g.at[0, X - 1], hvx.at[0, 1], 0, 1),
        send(v.at[0, 0], hvx.at[1, 0], 0, -1),
        send(g.at[0, 0], hvx.at[1, 1], 0, -1),
        send(vy_s.at[0], vy_r.at[0], 1, 1),
        send(vy_s.at[1], vy_r.at[1], 1, -1),
        send(vz_s.at[0], vz_r.at[0], 2, 1),
        send(vz_s.at[1], vz_r.at[1], 2, -1),
    ]
    if X > 1:
        loads[X - 1].wait()
        best = solve_layer(X - 1, best)
    x_copies = [
        send(nodes.at[1], nodes.at[X + 1], 0, -1),
        send(nodes.at[X], nodes.at[0], 0, 1),
    ]

    def lanes_of(chunk):
        return pl.ds(pl.multiple_of(chunk * LANES, LANES), LANES)

    def nodes_of(layer, zs):
        return (
            [nodes[layer, i, :, zs] for i in range(4)],
            [nodes[layer, 4 + i, :, zs] for i in range(4)],
        )

    for x in inner:
        loads[x].wait()
    if inner:
        best = lax.fori_loop(
            0, len(inner) * chunks,
            lambda i, b: solve(lax.div(i, chunks) + 1, lax.rem(i, chunks), b), best,
        )

    best = jnp.max(best, axis=0, keepdims=True)
    best = functools.reduce(
        jnp.maximum, [best[:, i : i + LANES] for i in range(0, JACOBI_LANES, LANES)]
    )
    peak[0] = best

    def spread_copy(buffer, which, offset):
        return pltpu.make_async_remote_copy(
            src_ref=buffer.at[0], dst_ref=buffer.at[offset],
            send_sem=all_send.at[which, offset], recv_sem=all_recv.at[which, offset],
            device_id=peer(offset), device_id_type=pl.DeviceIdType.MESH,
        )

    def spread(buffer, which):
        def one(offset, carry):
            spread_copy(buffer, which, offset).start()
            return carry

        lax.fori_loop(1, count, one, 0)

    def gathered(buffer, which):
        def one(offset, carry):
            spread_copy(buffer, which, offset).wait_recv()
            return carry

        lax.fori_loop(1, count, one, 0)

    for copy in velocity_copies[4:]:
        copy.wait_recv()

    zc = Z // LANES

    def side_faces(i, carry):
        x, chunk = lax.div(i, zc), lax.rem(i, zc)
        zs = lanes_of(chunk)
        w, s = nodes_of(x + 1, zs)
        vy, gy = v[1, x, :, zs], g[1, x, :, zs]
        up = [
            jnp.where(row == Y - 1, vy_r[1, x, part : part + 1, zs], pltpu.roll(a, Y - 1, 0))
            for part, a in ((0, vy), (1, gy))
        ]
        down = [
            jnp.where(row == 0, vy_r[0, x, part : part + 1, zs], pltpu.roll(a, 1, 0))
            for part, a in ((0, vy), (1, gy))
        ]
        high = outflow(w, s, 0.5 * (vy + up[0]), 0.5 * (gy + up[1]), jnp.maximum)
        for k in range(8):
            y_s[0, x, k : k + 1, zs] = high[k][Y - 1 : Y, :]
            acc[x, k, :, zs] = high[k] - jnp.where(row == 0, 0.0, pltpu.roll(high[k], 1, 0))
        low = outflow(w, s, 0.5 * (vy + down[0]), 0.5 * (gy + down[1]), jnp.minimum)
        for k in range(8):
            y_s[1, x, k : k + 1, zs] = low[k][0:1, :]
            acc[x, k, :, zs] += (
                jnp.where(row == Y - 1, 0.0, pltpu.roll(low[k], Y - 1, 0)) - low[k]
            )
        return carry

    lax.fori_loop(0, X * zc, side_faces, 0)
    spread(peak, 0)
    y_copies = [send(y_s.at[0], y_r.at[0], 1, 1), send(y_s.at[1], y_r.at[1], 1, -1)]

    def wall_faces(i, carry):
        x, chunk = lax.div(i, zc), lax.rem(i, zc)
        zs = lanes_of(chunk)
        nxt = lanes_of(lax.rem(chunk + 1, zc))
        prv = lanes_of(lax.rem(chunk + zc - 1, zc))
        w, s = nodes_of(x + 1, zs)
        final = chunk == zc - 1
        start = chunk == 0

        def means(ref, part):
            here = ref[2, x, :, zs]
            after = jnp.where(final, pltpu.roll(vz_r[1, x], LANES - part, 1), ref[2, x, :, nxt])
            ahead = jnp.where(
                start, pltpu.roll(vz_r[0, x], LANES - 1 - part, 1), ref[2, x, :, prv]
            )
            up = jnp.where(
                lane == LANES - 1, pltpu.roll(after, LANES - 1, 1), pltpu.roll(here, LANES - 1, 1)
            )
            down = jnp.where(lane == 0, pltpu.roll(ahead, 1, 1), pltpu.roll(here, 1, 1))
            return 0.5 * (here + up), 0.5 * (here + down)

        speeds, slopes = means(v, 0), means(g, 1)
        shut_high = (lane == LANES - 1) & (final & top)
        shut_low = (lane == 0) & (start & bottom)
        high = outflow(w, s, speeds[0], slopes[0], jnp.maximum)
        for k in range(8):
            zp[x, k, :, zs] = jnp.where(shut_high, 0.0, high[k])
        low = outflow(w, s, speeds[1], slopes[1], jnp.minimum)
        for k in range(8):
            zm[x, k, :, zs] = jnp.where(shut_low, 0.0, low[k])
        return carry

    lax.fori_loop(0, X * zc, wall_faces, 0)

    def pack_z(x, carry):
        high = jnp.zeros((Y, LANES), jnp.float32)
        low = jnp.zeros((Y, LANES), jnp.float32)
        for k in range(8):
            high = jnp.where(
                lane == k, pltpu.roll(zp[x, k, :, Z - LANES : Z], k + 1, 1), high
            )
            column = zm[x, k, :, 0:LANES]
            low = jnp.where(lane == k, pltpu.roll(column, k, 1) if k else column, low)
        z_s[0, x] = high
        z_s[1, x] = low
        return carry

    lax.fori_loop(0, X, pack_z, 0)

    def face_x(face, zs, left, right):
        speed, slope = 0.5 * (left[0] + right[0]), 0.5 * (left[1] + right[1])
        upper = outflow(*nodes_of(face, zs), speed, slope, jnp.maximum)
        lower = outflow(*nodes_of(face + 1, zs), speed, slope, jnp.minimum)
        for k in range(8):
            fx[face, k, :, zs] = upper[k] + lower[k]

    def drift_of(x, zs):
        return v[0, x, :, zs], g[0, x, :, zs]

    def inner_x(i, carry):
        face, zs = lax.div(i, zc) + 1, lanes_of(lax.rem(i, zc))
        face_x(face, zs, drift_of(face - 1, zs), drift_of(face, zs))
        return carry

    def outer_x(i, carry):
        zs = lanes_of(i)
        face_x(0, zs, (hvx[0, 0, :, zs], hvx[0, 1, :, zs]), drift_of(0, zs))
        face_x(X, zs, drift_of(X - 1, zs), (hvx[1, 0, :, zs], hvx[1, 1, :, zs]))
        return carry

    z_copies = [send(z_s.at[0], z_r.at[0], 2, 1), send(z_s.at[1], z_r.at[1], 2, -1)]
    if X > 1:
        lax.fori_loop(0, (X - 1) * zc, inner_x, 0)

    for copy in velocity_copies[:4] + x_copies:
        copy.wait_recv()
    lax.fori_loop(0, zc, outer_x, 0)
    for copy in y_copies + z_copies:
        copy.wait_recv()

    wide_row = lax.broadcasted_iota(jnp.int32, (Y, Z), 0)
    wide_lane = lax.broadcasted_iota(jnp.int32, (Y, Z), 1)

    def fold(value):
        value = functools.reduce(jnp.add, [value[i : i + 8, :] for i in range(0, Y, 8)])
        return functools.reduce(jnp.add, [value[:, i : i + LANES] for i in range(0, Z, LANES)])

    def combine(x, sums):
        fresh = []
        low_all, high_all = z_r[0, x], z_r[1, x]
        for k in range(8):
            fp, fm = zp[x, k], zm[x, k]
            first = pltpu.roll(low_all, LANES - k, 1) if k else low_all
            last = pltpu.roll(high_all, LANES - 1 - k, 1)
            spare = [first] * (Z // LANES - 1)
            before = jnp.where(
                wide_lane == 0, jnp.concatenate([first] + spare, 1), pltpu.roll(fp, 1, 1)
            )
            spare = [last] * (Z // LANES - 1)
            after = jnp.where(
                wide_lane == Z - 1, jnp.concatenate(spare + [last], 1), pltpu.roll(fm, Z - 1, 1)
            )
            change = acc[x, k] + ((fp + after) - (fm + before))
            change = change + (fx[x + 1, k] - fx[x, k])
            change = change + jnp.where(
                wide_row == Y - 1, y_r[1, x, k : k + 1, :],
                jnp.where(wide_row == 0, -y_r[0, x, k : k + 1, :], 0.0),
            )
            acc[x, k] = change
            fresh.append(sums[k] + fold(m[k, x]))
            fresh.append(sums[8 + k] + fold(change))
        return tuple(fresh[0::2] + fresh[1::2])

    zero = jnp.zeros((8, LANES), jnp.float32)
    sums = lax.fori_loop(0, X, combine, (zero,) * 16)

    one_lane = lax.broadcasted_iota(jnp.int32, (1, LANES), 1)
    packed = jnp.zeros((1, LANES), jnp.float32)
    for k in range(16):
        value = jnp.sum(jnp.sum(sums[k], axis=0, keepdims=True), axis=1, keepdims=True)
        packed = jnp.where(one_lane == k, value, packed)
    total[0] = packed
    gathered(peak, 0)
    largest = jnp.max(jnp.max(peak[...], axis=0), axis=1, keepdims=True)
    step = cfl_number / (largest + speed_eps)
    spread(total, 1)

    def update(x, carry):
        for k in range(8):
            out[k, x] = m[k, x] - step * acc[x, k]
        return carry

    lax.fori_loop(0, X, update, 0)
    gathered(total, 1)
    both = jnp.sum(total[...], axis=0)
    both = both - step * pltpu.roll(jnp.broadcast_to(both, (8, LANES)), LANES - 8, 1)[0:1]
    tot_ref[...] = both / float(count * X * Y * Z)

    for copy in sent:
        copy.wait_send()

    def drain(offset, carry):
        for which, buffer in ((0, peak), (1, total)):
            spread_copy(buffer, which, offset).wait_send()
        return carry

    lax.fori_loop(1, count, drain, 0)


def shards(sizes, moments, velocity, drift):
    _, X, Y, Z = moments.shape
    count = sizes[0] * sizes[1] * sizes[2]
    f32 = jnp.float32
    vm = lambda *shape: pltpu.VMEM(shape, f32)
    updated, totals = pl.pallas_call(
        functools.partial(kernel, sizes),
        name="transport",
        out_shape=(
            pltpu.VMEM(moments.shape, f32), pltpu.VMEM((1, LANES), f32)
        ),
        in_specs=[pl.BlockSpec(memory_space=pl.ANY)] * 3,
        out_specs=(
            pl.BlockSpec(memory_space=pltpu.VMEM), pl.BlockSpec(memory_space=pltpu.VMEM)
        ),
        scratch_shapes=[
            vm(8, X, Y, Z), vm(3, X, Y, Z), vm(3, X, Y, Z), vm(X + 2, 8, Y, Z), vm(X, 8, Y, Z),
            vm(X + 1, 8, Y, Z), vm(X, 8, Y, Z), vm(X, 8, Y, Z),
            vm(2, 2, Y, Z), vm(2, X, 2, Z), vm(2, X, 2, Z), vm(2, X, Y, LANES),
            vm(2, X, Y, LANES), vm(2, X, 8, Z), vm(2, X, 8, Z), vm(2, X, Y, LANES),
            vm(2, X, Y, LANES), vm(count, 1, LANES), vm(count, 1, LANES),
            pltpu.SemaphoreType.DMA((X + 2,)),
            pltpu.SemaphoreType.DMA((14,)), pltpu.SemaphoreType.DMA((14,)),
            pltpu.SemaphoreType.DMA((2, count)), pltpu.SemaphoreType.DMA((2, count)),
        ],
        compiler_params=pltpu.CompilerParams(collective_id=0, has_side_effects=True),
    )(moments, velocity, drift)
    return updated, totals[0, :8]


def solution(mesh):
    spec = P(None, "gx", "gy", "gz")
    sizes = tuple(mesh.shape[a] for a in AXES)
    return jax.shard_map(
        functools.partial(shards, sizes), mesh=mesh, in_specs=(spec,) * 3,
        out_specs=(spec, P()), check_vma=False,
    )
```

```python
import functools

import jax
import jax.numpy as jnp
from jax import lax
from jax.experimental import pallas as pl
from jax.experimental.pallas import tpu as pltpu
from jax.sharding import PartitionSpec as P

SWEEPS = 6
AXES = ("gx", "gy", "gz")
JACOBI_LANES = 512
LANES = 128

cfl_number = 0.4
speed_eps = 1e-06
pair_list = ((0, 1), (0, 2), (0, 3), (1, 2), (1, 3), (2, 3))


def entry_key(i, j):
    return (min(i, j), max(i, j))


def rotated(cosine, sine, near, far):
    if near is None and far is None:
        return None, None
    if near is None:
        return -(sine * far), cosine * far
    if far is None:
        return cosine * near, sine * near
    return cosine * near - sine * far, sine * near + cosine * far


def invert(moment):
    levels = list(moment)
    before = None
    inverse = 1.0 / levels[0]
    ratios = [levels[1] * inverse]
    alphas = [ratios[0]]
    betas = [levels[0]]
    for level in range(1, 4):
        fresh = [None] * 8
        for column in range(level, 8 - level):
            value = levels[column + 1] - alphas[level - 1] * levels[column]
            if level > 1:
                value = value - betas[level - 1] * before[column]
            fresh[column] = value
        betas.append(fresh[level] * inverse)
        inverse = 1.0 / fresh[level]
        ratios.append(fresh[level + 1] * inverse)
        alphas.append(ratios[level] - ratios[level - 1])
        before, levels = levels, fresh
    table = {(i, j): None for i in range(4) for j in range(i, 4)}
    for i in range(4):
        table[i, i] = alphas[i]
    for i in range(3):
        table[i, i + 1] = jnp.sqrt(betas[i + 1])
    first = [1.0, None, None, None]
    for _ in range(SWEEPS):
        for p, q in pair_list:
            coupling = table[p, q]
            if coupling is None:
                continue
            spread = table[q, q] - table[p, p]
            double = coupling + coupling
            r = lax.rsqrt(spread * spread + double * double)
            c2 = 0.5 + 0.5 * (jnp.abs(spread) * r)
            rc = lax.rsqrt(c2)
            cosine = c2 * rc
            signed = jnp.where(spread >= 0, coupling, -coupling)
            sine = signed * (r * rc)
            shift = sine * rc * coupling
            for rest in range(4):
                if rest not in (p, q):
                    a, b = entry_key(rest, p), entry_key(rest, q)
                    table[a], table[b] = rotated(cosine, sine, table[a], table[b])
            table[p, p] = table[p, p] - shift
            table[q, q] = table[q, q] + shift
            table[p, q] = None
            first[p], first[q] = rotated(cosine, sine, first[p], first[q])
    weights = [moment[0] * first[i] * first[i] for i in range(4)]
    return weights, [table[i, i] for i in range(4)]


def outflow(weights, sizes, mean_speed, mean_drift, upwind):
    sums = None
    for w, s in zip(weights, sizes):
        term = w * upwind(mean_speed + mean_drift * s, 0.0)
        terms = [term]
        for _ in range(7):
            term = term * s
            terms.append(term)
        sums = terms if sums is None else [a + b for a, b in zip(sums, terms)]
    return sums


def kernel(
    sizes, m_hbm, v_hbm, g_hbm, out, tot_ref,
    m, v, g, nodes, acc, fx, zp, zm,
    hvx, vy_s, vy_r, vz_s, vz_r, y_s, y_r, z_s, z_r, peak, total,
    in_sem, nb_send, nb_recv, all_send, all_recv,
):
    X, Y, Z = m.shape[1:]
    count = sizes[0] * sizes[1] * sizes[2]
    at = [lax.axis_index(a) for a in AXES]
    me = (at[0] * sizes[1] + at[1]) * sizes[2] + at[2]
    row = lax.broadcasted_iota(jnp.int32, (Y, LANES), 0)
    lane = lax.broadcasted_iota(jnp.int32, (Y, LANES), 1)
    bottom = at[2] == 0
    top = at[2] == sizes[2] - 1

    def peer(offset):
        where = lax.rem(me + offset, count)
        return (
            where // (sizes[1] * sizes[2]),
            lax.rem(where // sizes[2], sizes[1]),
            lax.rem(where, sizes[2]),
        )

    def beside(axis, step):
        place = list(at)
        place[axis] = lax.rem(at[axis] + step + sizes[axis], sizes[axis])
        return tuple(place)

    loads = [pltpu.make_async_copy(m_hbm.at[:, x], m.at[:, x], in_sem.at[x]) for x in range(X)]
    loads_v = pltpu.make_async_copy(v_hbm, v, in_sem.at[X])
    loads_g = pltpu.make_async_copy(g_hbm, g, in_sem.at[X + 1])
    edge = [0] if X == 1 else [0, X - 1]
    inner = list(range(1, X - 1))
    loads[0].start()
    loads_v.start()
    loads_g.start()
    for x in edge[1:] + inner:
        loads[x].start()

    barrier = pltpu.get_barrier_semaphore()

    def greet(offset, carry):
        pl.semaphore_signal(
            barrier, inc=1, device_id=peer(offset), device_id_type=pl.DeviceIdType.MESH
        )
        return carry

    lax.fori_loop(1, count, greet, 0)

    sent = []

    def send(src, dst, axis, step):
        index = len(sent)
        copy = pltpu.make_async_remote_copy(
            src_ref=src, dst_ref=dst, send_sem=nb_send.at[index], recv_sem=nb_recv.at[index],
            device_id=beside(axis, step), device_id_type=pl.DeviceIdType.MESH,
        )
        copy.start()
        sent.append(copy)
        return copy

    loads_v.wait()
    loads_g.wait()
    for x in range(X):
        for part, ref in ((0, v), (1, g)):
            vy_s[0, x, part : part + 1, :] = ref[1, x, Y - 1 : Y, :]
            vy_s[1, x, part : part + 1, :] = ref[1, x, 0:1, :]
        high = [ref[2, x, :, Z - LANES : Z] for ref in (v, g)]
        low = [ref[2, x, :, 0:LANES] for ref in (v, g)]
        vz_s[0, x] = jnp.where(lane == 0, pltpu.roll(high[0], 1, 1), pltpu.roll(high[1], 2, 1))
        vz_s[1, x] = jnp.where(lane == 0, low[0], pltpu.roll(low[1], 1, 1))

    chunks = Z // JACOBI_LANES

    def solve(x, chunk, best):
        zs = pl.ds(pl.multiple_of(chunk * JACOBI_LANES, JACOBI_LANES), JACOBI_LANES)
        weights, places = invert([m[k, x, :, zs] for k in range(8)])
        for i in range(4):
            nodes[x + 1, i, :, zs] = weights[i]
            nodes[x + 1, 4 + i, :, zs] = places[i]
        speed = None
        for d in range(3):
            vd, gd = v[d, x, :, zs], g[d, x, :, zs]
            parts = [jnp.abs(vd + gd * s) for s in places]
            largest = jnp.maximum(
                jnp.maximum(parts[0], parts[1]), jnp.maximum(parts[2], parts[3])
            )
            speed = largest if speed is None else speed + largest
        return jnp.maximum(best, speed)

    best = jnp.zeros((Y, JACOBI_LANES), jnp.float32)
    def solve_layer(x, best):
        return lax.fori_loop(0, chunks, lambda i, b: solve(x, i, b), best)

    loads[0].wait()
    best = solve_layer(0, best)
    pl.semaphore_wait(barrier, count - 1)
    velocity_copies = [
        send(v.at[0, X - 1], hvx.at[0, 0], 0, 1),
        send(g.at[0, X - 1], hvx.at[0, 1], 0, 1),
        send(v.at[0, 0], hvx.at[1, 0], 0, -1),
        send(g.at[0, 0], hvx.at[1, 1], 0, -1),
        send(vy_s.at[0], vy_r.at[0], 1, 1),
        send(vy_s.at[1], vy_r.at[1], 1, -1),
        send(vz_s.at[0], vz_r.at[0], 2, 1),
        send(vz_s.at[1], vz_r.at[1], 2, -1),
    ]
    if X > 1:
        loads[X - 1].wait()
        best = solve_layer(X - 1, best)
    x_copies = [
        send(nodes.at[1], nodes.at[X + 1], 0, -1),
        send(nodes.at[X], nodes.at[0], 0, 1),
    ]

    def lanes_of(chunk):
        return pl.ds(pl.multiple_of(chunk * LANES, LANES), LANES)

    def nodes_of(layer, zs):
        return (
            [nodes[layer, i, :, zs] for i in range(4)],
            [nodes[layer, 4 + i, :, zs] for i in range(4)],
        )

    for x in inner:
        loads[x].wait()
    if inner:
        best = lax.fori_loop(
            0, len(inner) * chunks,
            lambda i, b: solve(lax.div(i, chunks) + 1, lax.rem(i, chunks), b), best,
        )

    best = jnp.max(best, axis=0, keepdims=True)
    best = functools.reduce(
        jnp.maximum, [best[:, i : i + LANES] for i in range(0, JACOBI_LANES, LANES)]
    )
    peak[0] = best

    def spread_copy(buffer, which, offset):
        return pltpu.make_async_remote_copy(
            src_ref=buffer.at[0], dst_ref=buffer.at[offset],
            send_sem=all_send.at[which, offset], recv_sem=all_recv.at[which, offset],
            device_id=peer(offset), device_id_type=pl.DeviceIdType.MESH,
        )

    def spread(buffer, which):
        def one(offset, carry):
            spread_copy(buffer, which, offset).start()
            return carry

        lax.fori_loop(1, count, one, 0)

    def gathered(buffer, which):
        def one(offset, carry):
            spread_copy(buffer, which, offset).wait_recv()
            return carry

        lax.fori_loop(1, count, one, 0)

    for copy in velocity_copies[4:]:
        copy.wait_recv()

    zc = Z // LANES

    def side_faces(i, carry):
        x, chunk = lax.div(i, zc), lax.rem(i, zc)
        zs = lanes_of(chunk)
        w, s = nodes_of(x + 1, zs)
        vy, gy = v[1, x, :, zs], g[1, x, :, zs]
        up = [
            jnp.where(row == Y - 1, vy_r[1, x, part : part + 1, zs], pltpu.roll(a, Y - 1, 0))
            for part, a in ((0, vy), (1, gy))
        ]
        down = [
            jnp.where(row == 0, vy_r[0, x, part : part + 1, zs], pltpu.roll(a, 1, 0))
            for part, a in ((0, vy), (1, gy))
        ]
        high = outflow(w, s, 0.5 * (vy + up[0]), 0.5 * (gy + up[1]), jnp.maximum)
        for k in range(8):
            y_s[0, x, k : k + 1, zs] = high[k][Y - 1 : Y, :]
            acc[x, k, :, zs] = high[k] - jnp.where(row == 0, 0.0, pltpu.roll(high[k], 1, 0))
        low = outflow(w, s, 0.5 * (vy + down[0]), 0.5 * (gy + down[1]), jnp.minimum)
        for k in range(8):
            y_s[1, x, k : k + 1, zs] = low[k][0:1, :]
            acc[x, k, :, zs] += (
                jnp.where(row == Y - 1, 0.0, pltpu.roll(low[k], Y - 1, 0)) - low[k]
            )
        return carry

    lax.fori_loop(0, X * zc, side_faces, 0)
    spread(peak, 0)
    y_copies = [send(y_s.at[0], y_r.at[0], 1, 1), send(y_s.at[1], y_r.at[1], 1, -1)]

    def wall_faces(i, carry):
        x, chunk = lax.div(i, zc), lax.rem(i, zc)
        zs = lanes_of(chunk)
        nxt = lanes_of(lax.rem(chunk + 1, zc))
        prv = lanes_of(lax.rem(chunk + zc - 1, zc))
        w, s = nodes_of(x + 1, zs)
        final = chunk == zc - 1
        start = chunk == 0

        def means(ref, part):
            here = ref[2, x, :, zs]
            after = jnp.where(final, pltpu.roll(vz_r[1, x], LANES - part, 1), ref[2, x, :, nxt])
            ahead = jnp.where(
                start, pltpu.roll(vz_r[0, x], LANES - 1 - part, 1), ref[2, x, :, prv]
            )
            up = jnp.where(
                lane == LANES - 1, pltpu.roll(after, LANES - 1, 1), pltpu.roll(here, LANES - 1, 1)
            )
            down = jnp.where(lane == 0, pltpu.roll(ahead, 1, 1), pltpu.roll(here, 1, 1))
            return 0.5 * (here + up), 0.5 * (here + down)

        speeds, slopes = means(v, 0), means(g, 1)
        shut_high = (lane == LANES - 1) & (final & top)
        shut_low = (lane == 0) & (start & bottom)
        high = outflow(w, s, speeds[0], slopes[0], jnp.maximum)
        for k in range(8):
            zp[x, k, :, zs] = jnp.where(shut_high, 0.0, high[k])
        low = outflow(w, s, speeds[1], slopes[1], jnp.minimum)
        for k in range(8):
            zm[x, k, :, zs] = jnp.where(shut_low, 0.0, low[k])
        return carry

    lax.fori_loop(0, X * zc, wall_faces, 0)

    def pack_z(x, carry):
        high = jnp.zeros((Y, LANES), jnp.float32)
        low = jnp.zeros((Y, LANES), jnp.float32)
        for k in range(8):
            high = jnp.where(
                lane == k, pltpu.roll(zp[x, k, :, Z - LANES : Z], k + 1, 1), high
            )
            column = zm[x, k, :, 0:LANES]
            low = jnp.where(lane == k, pltpu.roll(column, k, 1) if k else column, low)
        z_s[0, x] = high
        z_s[1, x] = low
        return carry

    lax.fori_loop(0, X, pack_z, 0)

    def face_x(face, zs, left, right):
        speed, slope = 0.5 * (left[0] + right[0]), 0.5 * (left[1] + right[1])
        upper = outflow(*nodes_of(face, zs), speed, slope, jnp.maximum)
        lower = outflow(*nodes_of(face + 1, zs), speed, slope, jnp.minimum)
        for k in range(8):
            fx[face, k, :, zs] = upper[k] + lower[k]

    def drift_of(x, zs):
        return v[0, x, :, zs], g[0, x, :, zs]

    def inner_x(i, carry):
        face, zs = lax.div(i, zc) + 1, lanes_of(lax.rem(i, zc))
        face_x(face, zs, drift_of(face - 1, zs), drift_of(face, zs))
        return carry

    def outer_x(i, carry):
        zs = lanes_of(i)
        face_x(0, zs, (hvx[0, 0, :, zs], hvx[0, 1, :, zs]), drift_of(0, zs))
        face_x(X, zs, drift_of(X - 1, zs), (hvx[1, 0, :, zs], hvx[1, 1, :, zs]))
        return carry

    z_copies = [send(z_s.at[0], z_r.at[0], 2, 1), send(z_s.at[1], z_r.at[1], 2, -1)]
    if X > 1:
        lax.fori_loop(0, (X - 1) * zc, inner_x, 0)

    for copy in velocity_copies[:4] + x_copies:
        copy.wait_recv()
    lax.fori_loop(0, zc, outer_x, 0)
    for copy in y_copies + z_copies:
        copy.wait_recv()

    wide_row = lax.broadcasted_iota(jnp.int32, (Y, Z), 0)
    wide_lane = lax.broadcasted_iota(jnp.int32, (Y, Z), 1)

    def fold(value):
        value = functools.reduce(jnp.add, [value[i : i + 8, :] for i in range(0, Y, 8)])
        return functools.reduce(jnp.add, [value[:, i : i + LANES] for i in range(0, Z, LANES)])

    def combine(x, sums):
        fresh = []
        low_all, high_all = z_r[0, x], z_r[1, x]
        for k in range(8):
            fp, fm = zp[x, k], zm[x, k]
            first = pltpu.roll(low_all, LANES - k, 1) if k else low_all
            last = pltpu.roll(high_all, LANES - 1 - k, 1)
            spare = [first] * (Z // LANES - 1)
            before = jnp.where(
                wide_lane == 0, jnp.concatenate([first] + spare, 1), pltpu.roll(fp, 1, 1)
            )
            spare = [last] * (Z // LANES - 1)
            after = jnp.where(
                wide_lane == Z - 1, jnp.concatenate(spare + [last], 1), pltpu.roll(fm, Z - 1, 1)
            )
            change = acc[x, k] + ((fp + after) - (fm + before))
            change = change + (fx[x + 1, k] - fx[x, k])
            change = change + jnp.where(
                wide_row == Y - 1, y_r[1, x, k : k + 1, :],
                jnp.where(wide_row == 0, -y_r[0, x, k : k + 1, :], 0.0),
            )
            acc[x, k] = change
            fresh.append(sums[k] + fold(m[k, x]))
            fresh.append(sums[8 + k] + fold(change))
        return tuple(fresh[0::2] + fresh[1::2])

    zero = jnp.zeros((8, LANES), jnp.float32)
    sums = lax.fori_loop(0, X, combine, (zero,) * 16)

    one_lane = lax.broadcasted_iota(jnp.int32, (1, LANES), 1)
    packed = jnp.zeros((1, LANES), jnp.float32)
    for k in range(16):
        value = jnp.sum(jnp.sum(sums[k], axis=0, keepdims=True), axis=1, keepdims=True)
        packed = jnp.where(one_lane == k, value, packed)
    total[0] = packed
    spread(total, 1)
    gathered(peak, 0)
    largest = jnp.max(jnp.max(peak[...], axis=0), axis=1, keepdims=True)
    step = cfl_number / (largest + speed_eps)

    def update(x, carry):
        for k in range(8):
            out[k, x] = m[k, x] - step * acc[x, k]
        return carry

    lax.fori_loop(0, X, update, 0)
    gathered(total, 1)
    both = jnp.sum(total[...], axis=0)
    both = both - step * pltpu.roll(jnp.broadcast_to(both, (8, LANES)), LANES - 8, 1)[0:1]
    tot_ref[...] = both / float(count * X * Y * Z)

    for copy in sent:
        copy.wait_send()

    def drain(offset, carry):
        for which, buffer in ((0, peak), (1, total)):
            spread_copy(buffer, which, offset).wait_send()
        return carry

    lax.fori_loop(1, count, drain, 0)


def shards(sizes, moments, velocity, drift):
    _, X, Y, Z = moments.shape
    count = sizes[0] * sizes[1] * sizes[2]
    f32 = jnp.float32
    vm = lambda *shape: pltpu.VMEM(shape, f32)
    updated, totals = pl.pallas_call(
        functools.partial(kernel, sizes),
        name="transport",
        out_shape=(
            pltpu.VMEM(moments.shape, f32), pltpu.VMEM((1, LANES), f32)
        ),
        in_specs=[pl.BlockSpec(memory_space=pl.ANY)] * 3,
        out_specs=(
            pl.BlockSpec(memory_space=pltpu.VMEM), pl.BlockSpec(memory_space=pltpu.VMEM)
        ),
        scratch_shapes=[
            vm(8, X, Y, Z), vm(3, X, Y, Z), vm(3, X, Y, Z), vm(X + 2, 8, Y, Z), vm(X, 8, Y, Z),
            vm(X + 1, 8, Y, Z), vm(X, 8, Y, Z), vm(X, 8, Y, Z),
            vm(2, 2, Y, Z), vm(2, X, 2, Z), vm(2, X, 2, Z), vm(2, X, Y, LANES),
            vm(2, X, Y, LANES), vm(2, X, 8, Z), vm(2, X, 8, Z), vm(2, X, Y, LANES),
            vm(2, X, Y, LANES), vm(count, 1, LANES), vm(count, 1, LANES),
            pltpu.SemaphoreType.DMA((X + 2,)),
            pltpu.SemaphoreType.DMA((14,)), pltpu.SemaphoreType.DMA((14,)),
            pltpu.SemaphoreType.DMA((2, count)), pltpu.SemaphoreType.DMA((2, count)),
        ],
        compiler_params=pltpu.CompilerParams(collective_id=0, has_side_effects=True),
    )(moments, velocity, drift)
    return updated, totals[0, :8]


def solution(mesh):
    spec = P(None, "gx", "gy", "gz")
    sizes = tuple(mesh.shape[a] for a in AXES)
    return jax.shard_map(
        functools.partial(shards, sizes), mesh=mesh, in_specs=(spec,) * 3,
        out_specs=(spec, P()), check_vma=False,
    )
```
